128 devices in a mesh: dp: 4 (over z), expert: 16 (over y, x_hi, core), tensor: 2 (over x_lo).
Axes of the slice: x: 4 (x_hi: 2, x_lo: 2; x = x_hi * 2 + x_lo), y: 4, z: 4, core: 2. Of those that a mesh axis runs over, the one named last changes fastest.
Arguments:
- hidden: bfloat16 [8192, 6144], P(('dp', 'expert'), 'tensor'), may hold values from -6 to 6
- expert_ids: int32 [8192, 8], P(('dp', 'expert')), may hold values from 0 to 383, as said below
- gate_fixed: int32 [8192, 8], P(('dp', 'expert')), may hold values from 4096 to 65535
- slot_expert: int32 [64], replicated, may hold values from 0 to 383, as said below
- expert_in: bfloat16 [64, 6144, 2, 1024], P(('dp', 'expert'), 'tensor'), may hold values from -1 to 1, as said below
- expert_out: bfloat16 [64, 1024, 6144], P(('dp', 'expert'), None, 'tensor'), may hold values from -1 to 1, as said below
- shared_in: bfloat16 [6144, 2, 1024], P('tensor', None, 'dp'), may hold values from -0.078125 to 0.078125
- shared_out: bfloat16 [1024, 6144], P('dp', 'tensor'), may hold values from -0.1875 to 0.1875
Outputs:
- mixed: bfloat16 [8192, 6144], P(('dp', 'expert'), 'tensor')
The draws below stay inside these ranges and needn't reach their ends.
Inputs may be any that keep to these rules, and one draw needn't show every extreme that they name: `expert_ids`: each row names 8 different experts. `slot_expert`: 56 different experts fill the 64 slots; 8 of them hold two slots each, the others one. `expert_in`: slots that hold the same expert hold the same weights. `expert_out`: slots that hold the same expert hold the same weights.
All inputs are finite; a program needn't handle non-finite values.
Results may differ from the reference program's by a relative error of at most 0.006.
Values may be sent and summed in bfloat16 or wider, within the bound.
No kernel may reach another device: no remote copies, remote signals or barrier semaphores. Data moves between devices by JAX's collectives and lax.ppermute only.
A program may use at most 192 MiB of HBM per device.

```python
import jax
import jax.numpy as jnp
from jax import lax

D = 6144
FF_E = 1024
FF_S = 1024
EXPERTS = 384
TOPK = 8
CAP = 4
TOK_DEV = 128
SLOTS = 64
REPL = 8
WIN = 56
TOKENS = 8192


def routing_plan(key):
    base = jax.random.fold_in(key, 4242)
    key_bias, key_noise, key_pick, key_perm = jax.random.split(base, 4)
    order = jnp.arange(EXPERTS, dtype=jnp.int32)
    level = jax.random.randint(key_bias, (EXPERTS,), 0, 8, dtype=jnp.int32)
    bias = level * level
    noise = jax.random.randint(key_noise, (TOKENS, EXPERTS), 0, 1024, dtype=jnp.int32)
    score = (noise + bias[None, :]) * EXPERTS + order[None, :]
    _, chosen = lax.top_k(score, TOPK)
    pick = jax.random.randint(key_pick, (EXPERTS,), 0, 1 << 20, dtype=jnp.int32) * EXPERTS + order
    ends = (order == 0) | (order == EXPERTS - 1)
    pick = jnp.where(ends, (1 << 21) * EXPERTS + order, pick).astype(jnp.int32)
    _, resident = lax.top_k(pick, WIN)
    heat = bias[resident] * EXPERTS + resident
    _, hot_place = lax.top_k(heat, REPL)
    entries = jnp.concatenate([jnp.arange(WIN, dtype=jnp.int32), hot_place.astype(jnp.int32)])
    shuffle = jax.random.permutation(key_perm, SLOTS)
    slot_resident = entries[shuffle]
    return (chosen.astype(jnp.int32), resident[slot_resident].astype(jnp.int32), slot_resident)


def expert_weights(key, salt, shape, fan_in):
    _, _, slot_resident = routing_plan(key)
    weight_key = jax.random.fold_in(key, salt)
    factor = fan_in ** (-0.5)

    def one_slot(resident_index):
        values = jax.random.truncated_normal(jax.random.fold_in(weight_key, resident_index), -4.0, 4.0, shape, jnp.float32)
        return (values * factor).astype(jnp.bfloat16)
    return lax.map(one_slot, slot_resident)


def draw_expert_ids(key, part):
    return routing_plan(key)[0]


def draw_slot_expert(key, part):
    return routing_plan(key)[1]


def draw_expert_in(key, part):
    return expert_weights(key, 17, (D, 2, FF_E), D)


def draw_expert_out(key, part):
    return expert_weights(key, 29, (FF_E, D), FF_E)


def touch_ends(array, own_key, low, high):
    dims = array.shape
    place = [jax.random.randint(jax.random.fold_in(own_key, axis), (), 0, dims[axis]) for axis in range(len(dims))]
    array = array.at[tuple(place)].set(low)
    longest = dims.index(max(dims))
    place[longest] = (place[longest] + 1) % dims[longest]
    return array.at[tuple(place)].set(high)


def steps_of(own_key, shape, cuts, smallest, high):
    def one(position, parts):
        heights = jax.random.uniform(jax.random.fold_in(jax.random.fold_in(own_key, 6), position), (parts,), jnp.float32, smallest / len(cuts), high / len(cuts))
        return jnp.repeat(jnp.exp(heights), shape[position] // parts).reshape((-1,) + (1,) * (len(shape) - position - 1))

    loudness = one(*cuts[0])
    for cut in cuts[1:]:
        loudness = loudness * one(*cut)
    return loudness


def scatter_about(rng, shape, width, bound, shards=(), kind=jnp.bfloat16):
    drawn = width * jax.random.normal(rng, shape, jnp.float32)
    if shards:
        drawn = drawn * steps_of(rng, shape, shards, -0.22, 0.18)
    return jnp.clip(drawn, -bound, bound).astype(kind)


def setup_inputs(seed: int = 0) -> dict:
    keys = jax.random.split(jax.random.key(seed), 9)
    hidden = scatter_about(keys[0], (TOKENS, D), 1.0, 6.0, ((0, 64), (1, 2)))
    expert_ids = draw_expert_ids(jax.random.fold_in(keys[8], 71), 0)
    gate_fixed = touch_ends(jax.random.randint(keys[2], (TOKENS, TOPK), 4096, 65536), jax.random.fold_in(keys[2], 1), 4096, 65535).astype(jnp.int32)
    slot_expert = draw_slot_expert(jax.random.fold_in(keys[8], 71), 0)
    expert_in = draw_expert_in(jax.random.fold_in(keys[8], 71), 0)
    expert_out = draw_expert_out(jax.random.fold_in(keys[8], 71), 0)
    shared_in = scatter_about(keys[6], (D, 2, FF_S), D ** -0.5, 0.078125, ((0, 2), (2, 4)))
    shared_out = scatter_about(keys[7], (FF_S, D), FF_S ** -0.5, 0.1875, ((0, 4), (1, 2)))
    return dict(hidden=hidden, expert_ids=expert_ids, gate_fixed=gate_fixed, slot_expert=slot_expert, expert_in=expert_in, expert_out=expert_out, shared_in=shared_in, shared_out=shared_out)


gate_scale = 1.0 / 65536.0


def swiglu(pre):
    return (jax.nn.silu(pre[:, 0, :]) * pre[:, 1, :]).astype(jnp.bfloat16)


def route_plan(chosen, row_rank, slot_expert):
    slot_count = slot_expert.shape[0]
    slot_iota = jnp.arange(slot_count, dtype=jnp.int32)[:, None]
    owns = slot_expert[:, None] == jnp.arange(chosen.shape[2], dtype=jnp.int32)[None, :]
    home = jnp.min(jnp.where(owns, slot_iota, slot_count), axis=0).astype(jnp.int32)
    spare = jnp.min(jnp.where(owns & (slot_iota != home[None, :]), slot_iota, slot_count), axis=0).astype(jnp.int32)
    home_of = jnp.sum(jnp.where(chosen, home[None, None, :], 0), axis=2).astype(jnp.int32)
    spare_of = jnp.sum(jnp.where(chosen, spare[None, None, :], 0), axis=2).astype(jnp.int32)
    first = row_rank < CAP
    spill = (row_rank >= CAP) & (row_rank < 2 * CAP) & (spare_of < slot_count)
    target = jnp.where(first, home_of, jnp.where(spill, spare_of, slot_count)).astype(jnp.int32)
    slot_row = jnp.where(first, row_rank, row_rank - CAP).astype(jnp.int32)
    return target, slot_row


def reference(hidden, expert_ids, gate_fixed, slot_expert, expert_in, expert_out, shared_in, shared_out):
    tokens_all = hidden.shape[0]
    slot_count = slot_expert.shape[0]
    blocks = tokens_all // TOK_DEV
    experts_iota = jnp.arange(EXPERTS, dtype=jnp.int32)
    chosen = expert_ids[:, :, None] == experts_iota[None, None, :]
    picked = jnp.any(chosen, axis=1).astype(jnp.int32).reshape(blocks, TOK_DEV, EXPERTS)
    before = (jnp.cumsum(picked, axis=1) - picked).astype(jnp.int32).reshape(tokens_all, EXPERTS)
    row_rank = jnp.sum(jnp.where(chosen, before[:, None, :], 0), axis=2).astype(jnp.int32)
    target, slot_row = route_plan(chosen, row_rank, slot_expert)
    token_iota = jnp.arange(tokens_all, dtype=jnp.int32)
    token_block = token_iota // TOK_DEV
    buffer_size = slot_count * blocks * CAP
    flat = jnp.where(target < slot_count, (target * blocks + token_block[:, None]) * CAP + slot_row, buffer_size).astype(jnp.int32)
    owner = jnp.broadcast_to(token_iota[:, None], flat.shape).astype(jnp.int32)
    table = jnp.full((buffer_size + 1,), tokens_all, jnp.int32).at[flat.reshape(-1)].set(owner.reshape(-1))
    table = table[:buffer_size].reshape(slot_count, blocks * CAP)
    padded = jnp.concatenate([hidden, jnp.zeros((1, D), hidden.dtype)], axis=0)

    def expert_pass(item):
        rows_index, weight_in, weight_out = item
        rows = padded[rows_index]
        pre = jnp.dot(rows, weight_in.reshape(D, 2 * FF_E), preferred_element_type=jnp.float32).reshape(-1, 2, FF_E)
        return jnp.dot(swiglu(pre), weight_out, preferred_element_type=jnp.float32).astype(jnp.bfloat16)

    answers = lax.map(expert_pass, (table, expert_in, expert_out)).reshape(buffer_size, D)
    answers = jnp.concatenate([answers, jnp.zeros((1, D), answers.dtype)], axis=0)
    gates = gate_fixed.astype(jnp.float32) * gate_scale
    routed = jnp.zeros((tokens_all, D), jnp.float32)
    for column in range(TOPK):
        routed = routed + gates[:, column:column + 1] * answers[flat[:, column]].astype(jnp.float32)
    shared_pre = jnp.dot(hidden, shared_in.reshape(D, 2 * FF_S), preferred_element_type=jnp.float32).reshape(-1, 2, FF_S)
    shared = jnp.dot(swiglu(shared_pre), shared_out, preferred_element_type=jnp.float32)
    return (shared + routed).astype(jnp.bfloat16)
```

```python
import functools

import jax
import jax.numpy as jnp
from jax import lax
from jax.experimental import pallas as pl
from jax.experimental.pallas import tpu as pltpu
from jax.sharding import PartitionSpec as P

CAP = 4
BF = jnp.bfloat16
F32 = jnp.float32


def params():
    return pltpu.CompilerParams(vmem_limit_bytes=50 * 2**20)


def dot(a, b):
    return jnp.dot(a, b, preferred_element_type=F32)


def iota(shape, dim):
    return lax.broadcasted_iota(jnp.int32, shape, dim)


def silu_mul(gate, up):
    return (jax.nn.silu(gate) * up).astype(BF)


def route_kernel(ids, gates, experts, experts_col, hidden, rows_out, high_out, low_out):
    tokens = ids.shape[0]
    lanes = experts.shape[1]
    slots = experts_col.shape[0]
    half = hidden.shape[1] // 2
    held = experts[...]
    named = jnp.zeros((tokens, lanes), jnp.bool_)
    gate = jnp.zeros((tokens, lanes), jnp.int32)
    for k in range(ids.shape[1]):
        hit = ids[:, k : k + 1] == held
        named = named | hit
        gate = gate + jnp.where(hit, gates[:, k : k + 1], 0)
    lane = iota((slots, lanes), 1)
    twin = (experts_col[...] == held) & (iota((slots, lanes), 0) < lane // (2 * CAP))
    spare = jnp.max(jnp.where(twin, CAP, 0), axis=0, keepdims=True)
    earlier = iota((tokens, tokens), 0) > iota((tokens, tokens), 1)
    rank = dot(
        jnp.where(earlier, 1.0, 0.0).astype(BF), jnp.where(named, 1.0, 0.0).astype(BF)
    ).astype(jnp.int32)
    lane = iota((tokens, lanes), 1)
    served = named & (rank - spare == lane % CAP)
    left = lane % (2 * CAP) < CAP
    pick_left = jnp.where(served & left, 1.0, 0.0).astype(BF)
    pick_right = jnp.where(served & ~left, 1.0, 0.0).astype(BF)
    high = jnp.where(served, gate // 256, 0).astype(F32) * 2.0**-8
    low = jnp.where(served, gate % 256, 0).astype(F32) * 2.0**-16
    high_out[...] = high.astype(BF)
    low_out[...] = low.astype(BF)
    across = (((0,), (0,)), ((), ()))
    rows = lax.dot_general(pick_left, hidden[:, :half], across, preferred_element_type=F32)
    rows += lax.dot_general(pick_right, hidden[:, half:], across, preferred_element_type=F32)
    rows_out[...] = rows.astype(BF)


def route(ids, gates, slot_expert, hidden):
    slots = slot_expert.shape[0]
    lanes = slots * 2 * CAP
    tokens, width = hidden.shape
    return pl.pallas_call(
        route_kernel,
        out_shape=(
            jax.ShapeDtypeStruct((lanes, width // 2), BF),
            jax.ShapeDtypeStruct((tokens, lanes), BF),
            jax.ShapeDtypeStruct((tokens, lanes), BF),
        ),
        compiler_params=params(),
        name="route",
    )(ids, gates, jnp.repeat(slot_expert, 2 * CAP)[None], slot_expert[:, None], hidden)


def split_kernel(w, out):
    depth, _, units = w.shape
    rows = w[...].reshape(2 * depth, units)
    row, col = iota((2 * depth, 2 * depth), 0), iota((2 * depth, 2 * depth), 1)
    source = jnp.where(row < depth, 2 * row, 2 * (row - depth) + 1)
    moved = dot(jnp.where(col == source, 1.0, 0.0).astype(BF), rows).astype(BF)
    out[:, :units] = moved[:depth]
    out[:, units:] = moved[depth:]


def split_gate_up(w, depth=256):
    width, _, units = w.shape
    return pl.pallas_call(
        split_kernel,
        grid=(width // depth,),
        in_specs=[pl.BlockSpec((depth, 2, units), lambda i: (i, 0, 0))],
        out_specs=pl.BlockSpec((depth, 2 * units), lambda i: (i, 0)),
        out_shape=jax.ShapeDtypeStruct((width, 2 * units), BF),
        compiler_params=params(),
        name="split",
    )(w)


def unfold_kernel(me, arrived, w, x_out, part_out):
    @pl.when(pl.program_id(0) == 0)
    def _():
        half = arrived.shape[1]
        rows = arrived.shape[0] // 2
        row, col = iota((rows, 2 * rows), 0), iota((rows, 2 * rows), 1)
        first = row // CAP * (2 * CAP) + row % CAP
        for h in range(2):
            pick = jnp.where(col == first + h * CAP, 1.0, 0.0).astype(BF)
            x_out[:, h * half : (h + 1) * half] = dot(pick, arrived[...]).astype(BF)

    part_out[...] = dot(x_out[...], w[...]).astype(part_out.dtype)


def half_block(j, mine, blocks):
    return j // blocks * 2 * blocks + mine * blocks + j % blocks


def send_half(arrived, w, me, block=256):
    lanes, half = arrived.shape
    rows, units = lanes // 2, w.shape[1] // 2
    blocks = units // 2 // block
    return pl.pallas_call(
        unfold_kernel,
        grid_spec=pltpu.PrefetchScalarGridSpec(
            num_scalar_prefetch=1,
            grid=(2 * blocks,),
            in_specs=[
                pl.BlockSpec((lanes, half), lambda j, me: (0, 0)),
                pl.BlockSpec(
                    (2 * half, block), lambda j, me: (0, half_block(j, 1 - me[0], blocks))
                ),
            ],
            out_specs=(
                pl.BlockSpec((rows, 2 * half), lambda j, me: (0, 0)),
                pl.BlockSpec((rows, block), lambda j, me: (0, j)),
            ),
        ),
        out_shape=(
            jax.ShapeDtypeStruct((rows, 2 * half), BF),
            jax.ShapeDtypeStruct((rows, units), BF),
        ),
        compiler_params=params(),
        name="send_half",
    )(me, arrived, w)


def keep_kernel(me, x, w, out):
    out[...] = dot(x[...], w[...])


def keep_half(x, w, me, block=256):
    rows, width = x.shape
    units = w.shape[1] // 2
    blocks = units // 2 // block
    return pl.pallas_call(
        keep_kernel,
        grid_spec=pltpu.PrefetchScalarGridSpec(
            num_scalar_prefetch=1,
            grid=(2 * blocks,),
            in_specs=[
                pl.BlockSpec((rows, width), lambda j, me: (0, 0)),
                pl.BlockSpec((width, block), lambda j, me: (0, half_block(j, me[0], blocks))),
            ],
            out_specs=pl.BlockSpec((rows, block), lambda j, me: (0, j)),
        ),
        out_shape=jax.ShapeDtypeStruct((rows, units), F32),
        compiler_params=params(),
        name="keep_half",
    )(me, x, w)


def act_kernel(kept, came, out):
    units = out.shape[1]
    pre = kept[...] + came[...].astype(F32)
    out[...] = silu_mul(pre[:, :units], pre[:, units:])


def activate(kept, came):
    rows, units = kept.shape
    return pl.pallas_call(
        act_kernel,
        out_shape=jax.ShapeDtypeStruct((rows, units // 2), BF),
        compiler_params=params(),
        name="activate",
    )(kept, came)


def answer_kernel(me, mine, other, w_mine_l, w_other_l, w_mine_r, w_other_r, out):
    rows = mine.shape[0]
    row, col = iota((2 * rows, rows), 0), iota((2 * rows, rows), 1)
    first = col // CAP * (2 * CAP) + col % CAP
    total = jnp.zeros(out.shape, F32)
    for h, (wm, wo) in enumerate(((w_mine_l, w_other_l), (w_mine_r, w_other_r))):
        answer = (dot(mine[...], wm[...]) + dot(other[...], wo[...])).astype(BF)
        total += dot(jnp.where(row == first + h * CAP, 1.0, 0.0).astype(BF), answer)
    out[...] = total.astype(BF)


def answers(mine, other, w, me, block=512):
    rows, units = mine.shape
    width = w.shape[1]
    blocks = width // 2 // block

    def part(side, h):
        return pl.BlockSpec(
            (units, block),
            lambda n, me: ((me[0] if side else 1 - me[0]), h * blocks + n),
        )

    whole = pl.BlockSpec((rows, units), lambda n, me: (0, 0))
    return pl.pallas_call(
        answer_kernel,
        grid_spec=pltpu.PrefetchScalarGridSpec(
            num_scalar_prefetch=1,
            grid=(blocks,),
            in_specs=[whole, whole, part(1, 0), part(0, 0), part(1, 1), part(0, 1)],
            out_specs=pl.BlockSpec((2 * rows, block), lambda n, me: (0, n)),
        ),
        out_shape=jax.ShapeDtypeStruct((2 * rows, width // 2), BF),
        compiler_params=params(),
        name="answers",
    )(me, mine, other, w, w, w, w)


def shared_kernel(me, own, prev, nxt, far_a, far_b, w, sent, kept):
    units = w.shape[1] // 4
    rows = own.shape[0]
    for i, piece in enumerate((own, prev, nxt)):
        pre = dot(piece[...], w[...])
        store_shared(me, pre, sent, kept, i * rows, rows, units)
    for i, piece in enumerate((far_a, far_b)):
        pre = dot(piece[...], w[...])
        store_shared(me, pre, sent, kept, 3 * rows + i * (rows // 2), rows // 2, units)


def store_shared(me, pre, sent, kept, start, rows, units):
    first = jnp.concatenate([pre[:, :units], pre[:, 2 * units : 3 * units]], axis=1)
    second = jnp.concatenate([pre[:, units : 2 * units], pre[:, 3 * units :]], axis=1)
    low = me[0] == 0
    kept[start : start + rows, :] = jnp.where(low, first, second)
    sent[start : start + rows, :] = jnp.where(low, second, first).astype(BF)


def shared_in_half(pieces, w, me):
    rows = pieces[0].shape[0]
    out = w.shape[1] // 2
    return pl.pallas_call(
        shared_kernel,
        in_specs=[pl.BlockSpec(memory_space=pltpu.SMEM)]
        + [pl.BlockSpec(memory_space=pltpu.VMEM)] * 6,
        out_shape=(
            jax.ShapeDtypeStruct((4 * rows, out), BF),
            jax.ShapeDtypeStruct((4 * rows, out), F32),
        ),
        compiler_params=params(),
        name="shared_in",
    )(me, *pieces, w)


def far_kernel(me, mine, other, w, up, down):
    units = mine.shape[1]
    rows = mine.shape[0] // 4
    low = me[0] == 0
    m, o = mine[3 * rows :, :], other[3 * rows :, :]
    act = jnp.where(low, jnp.concatenate([m, o], axis=1), jnp.concatenate([o, m], axis=1))
    total = dot(act, w[...])
    up[...] = total[: rows // 2].astype(BF)
    down[...] = total[rows // 2 :].astype(BF)


def shared_far(mine, other, w, me):
    rows, width = mine.shape[0] // 4, w.shape[1]
    half = jax.ShapeDtypeStruct((rows // 2, width), BF)
    return pl.pallas_call(
        far_kernel,
        in_specs=[pl.BlockSpec(memory_space=pltpu.SMEM)]
        + [pl.BlockSpec(memory_space=pltpu.VMEM)] * 3,
        out_shape=(half, half),
        compiler_params=params(),
        name="shared_far",
    )(me, mine, other, w)


def near_kernel(me, mine, other, w, came_up, came_down, up, down):
    rows = mine.shape[0] // 4
    low = me[0] == 0
    m, o = mine[rows : 3 * rows, :], other[rows : 3 * rows, :]
    act = jnp.where(low, jnp.concatenate([m, o], axis=1), jnp.concatenate([o, m], axis=1))
    total = dot(act, w[...])
    h = rows // 2
    down[:h, :] = total[:h].astype(BF)
    down[h:, :] = (total[h:rows] + came_down[...].astype(F32)).astype(BF)
    up[:h, :] = (total[rows : rows + h] + came_up[...].astype(F32)).astype(BF)
    up[h:, :] = total[rows + h :].astype(BF)


def shared_near(mine, other, w, came_up, came_down, me):
    rows, width = mine.shape[0] // 4, w.shape[1]
    full = jax.ShapeDtypeStruct((rows, width), BF)
    return pl.pallas_call(
        near_kernel,
        in_specs=[pl.BlockSpec(memory_space=pltpu.SMEM)]
        + [pl.BlockSpec(memory_space=pltpu.VMEM)] * 5,
        out_shape=(full, full),
        compiler_params=params(),
        name="shared_near",
    )(me, mine, other, w, came_up, came_down)


def mix_kernel(me, high, low, back, mine, other, w, from_prev, from_next, out):
    half = back.shape[1]
    lane = iota(high.shape, 1)
    is_low = me[0] == 0
    tokens = out.shape[0]
    m, o = mine[:tokens, :], other[:tokens, :]
    act = jnp.where(is_low, jnp.concatenate([m, o], axis=1), jnp.concatenate([o, m], axis=1))
    for h in range(2):
        cols = slice(h * half, (h + 1) * half)
        here = lane % (2 * CAP) // CAP == h
        zero = jnp.zeros((), BF)
        routed = dot(jnp.where(here, high[...], zero), back[...])
        routed += dot(jnp.where(here, low[...], zero), back[...])
        shared = dot(act, w[:, cols])
        shared += from_prev[:, cols].astype(F32) + from_next[:, cols].astype(F32)
        out[:, cols] = (shared + routed).astype(BF)


def mix(high, low, back, mine, other, w, from_prev, from_next, me):
    tokens, lanes = high.shape
    width = w.shape[1]
    whole = pl.BlockSpec(memory_space=pltpu.VMEM)
    return pl.pallas_call(
        mix_kernel,
        in_specs=[pl.BlockSpec(memory_space=pltpu.SMEM)] + [whole] * 8,
        out_shape=jax.ShapeDtypeStruct((tokens, width), BF),
        compiler_params=params(),
        name="mix",
    )(me, high, low, back, mine, other, w, from_prev, from_next)


def shift(array, axis, by):
    size = lax.axis_size(axis)
    return lax.ppermute(array, axis, [(i, (i + by) % size) for i in range(size)])


def exchange(rows):
    return lax.all_to_all(rows, ("dp", "expert"), split_axis=0, concat_axis=0, tiled=True)


def shards(
    hidden, expert_ids, gate_fixed, slot_expert, expert_in, expert_out, shared_in, shared_out
):
    tokens, width = hidden.shape
    slots = slot_expert.shape[0]
    half = width // 2
    me = lax.axis_index("tensor").astype(jnp.int32)[None]

    prev = shift(hidden, "dp", 1)
    nxt = shift(hidden, "dp", -1)
    send_rows, high, low = route(expert_ids, gate_fixed, slot_expert, hidden)
    arrived = exchange(send_rows.reshape(slots, 2 * CAP, half)).reshape(-1, half)
    far_a = shift(prev[: tokens // 2], "dp", 1)
    far_b = shift(nxt[tokens // 2 :], "dp", -1)
    w_in = split_gate_up(expert_in[0])
    w_shared = split_gate_up(shared_in)

    x, sent = send_half(arrived, w_in, me)
    came = shift(sent, "tensor", 1)
    kept = keep_half(x, w_in, me)
    act = activate(kept, came)
    act_other = shift(act, "tensor", 1)
    back = exchange(
        answers(act, act_other, expert_out[0], me).reshape(slots, 2 * CAP, half)
    ).reshape(-1, half)

    s_sent, s_kept = shared_in_half((hidden, prev, nxt, far_a, far_b), w_shared, me)
    s_came = shift(s_sent, "tensor", 1)
    s_act = activate(s_kept, s_came)
    s_other = shift(s_act, "tensor", 1)
    up, down = shared_far(s_act, s_other, shared_out, me)
    came_up = shift(up, "dp", 1)
    came_down = shift(down, "dp", -1)
    up, down = shared_near(s_act, s_other, shared_out, came_up, came_down, me)
    from_prev = shift(up, "dp", 1)
    from_next = shift(down, "dp", -1)
    return mix(high, low, back, s_act, s_other, shared_out, from_prev, from_next, me)


def solution(mesh):
    in_specs = (
        P(("dp", "expert"), "tensor"),
        P(("dp", "expert"), None),
        P(("dp", "expert"), None),
        P(),
        P(("dp", "expert"), "tensor", None, None),
        P(("dp", "expert"), None, "tensor"),
        P("tensor", None, "dp"),
        P("dp", "tensor"),
    )
    out_specs = P(("dp", "expert"), "tensor")
    return jax.shard_map(shards, mesh=mesh, in_specs=in_specs, out_specs=out_specs, check_vma=False)
```

```python
import functools

import jax
import jax.numpy as jnp
from jax import lax
from jax.experimental import pallas as pl
from jax.experimental.pallas import tpu as pltpu
from jax.sharding import PartitionSpec as P


CAP = 4
BF = jnp.bfloat16
F32 = jnp.float32


def params(mib=20):
    return pltpu.CompilerParams(vmem_limit_bytes=mib * 2**20)


def far(array):
    return pltpu.with_memory_space_constraint(array, pltpu.HBM)


def dot(a, b):
    return jnp.dot(a, b, preferred_element_type=F32)


def iota(shape, dim):
    return lax.broadcasted_iota(jnp.int32, shape, dim)


def silu_mul(gate, up):
    return (jax.nn.silu(gate) * up).astype(BF)


def route_kernel(ids, gates, held_row, left, right, rows_out, high_out, low_out, pick):
    slots = held_row.shape[1]
    fold = 2 * CAP
    lanes = slots * fold
    tokens = ids.shape[1]

    @pl.when(pl.program_id(0) == 0)
    def _():
        row, col = iota((lanes, slots), 0), iota((lanes, slots), 1)
        held_all = jnp.broadcast_to(held_row[...], (lanes, slots))
        held = jnp.max(jnp.where(col == row // fold, held_all, -1), axis=1, keepdims=True)
        twin = (held_all == held) & (col < row // fold)
        spare = jnp.max(jnp.where(twin, CAP, 0), axis=1, keepdims=True)
        named = jnp.zeros((lanes, tokens), jnp.float32)
        gate = jnp.zeros((lanes, tokens), jnp.int32)
        for k in range(ids.shape[0]):
            hit = ids[k : k + 1, :] == held
            named = jnp.where(hit, 1.0, named)
            gate = gate + jnp.where(hit, gates[k : k + 1, :], 0)
        earlier = iota((tokens, tokens), 0) < iota((tokens, tokens), 1)
        rank = dot(named.astype(BF), jnp.where(earlier, 1.0, 0.0).astype(BF)).astype(jnp.int32)
        row = iota((lanes, tokens), 0)
        served = (named > 0.5) & (rank - spare == row % CAP)
        is_left = row % fold < CAP
        pick[0] = jnp.where(served & is_left, 1.0, 0.0).astype(BF)
        pick[1] = jnp.where(served & ~is_left, 1.0, 0.0).astype(BF)
        high = jnp.where(served, gate // 256, 0).astype(F32) * 2.0**-8
        low = jnp.where(served, gate % 256, 0).astype(F32) * 2.0**-16
        high_out[...] = high.astype(BF)
        low_out[...] = low.astype(BF)

    rows_out[...] = (dot(pick[0], left[...]) + dot(pick[1], right[...])).astype(BF)


def route(ids, gates, slot_expert, hidden, block=512):
    slots = slot_expert.shape[0]
    lanes = slots * 2 * CAP
    tokens, width = hidden.shape
    half = width // 2
    blocks = half // block

    def whole(*shape):
        return pl.BlockSpec(shape, lambda j: (0, 0))

    return pl.pallas_call(
        route_kernel,
        grid=(blocks,),
        in_specs=[
            whole(ids.shape[1], tokens),
            whole(ids.shape[1], tokens),
            whole(1, slots),
            pl.BlockSpec((tokens, block), lambda j: (0, j)),
            pl.BlockSpec((tokens, block), lambda j: (0, blocks + j)),
        ],
        out_specs=(
            pl.BlockSpec((lanes, block), lambda j: (0, j)),
            whole(lanes, tokens),
            whole(lanes, tokens),
        ),
        out_shape=(
            pltpu.HBM((lanes, half), BF),
            pltpu.HBM((lanes, tokens), BF),
            pltpu.HBM((lanes, tokens), BF),
        ),
        scratch_shapes=[pltpu.VMEM((2, lanes, tokens), BF)],
        compiler_params=params(16),
        name="route",
    )(*(far(x) for x in (ids.T, gates.T, slot_expert[None], hidden, hidden)))


def split_kernel(w, out, *, sub, paired):
    depth, _, units = w.shape
    blocks, _, block = out.shape
    row, col = iota((2 * sub, 2 * sub), 0), iota((2 * sub, 2 * sub), 1)
    source = jnp.where(row < sub, 2 * row, 2 * (row - sub) + 1)
    order = jnp.where(col == source, 1.0, 0.0).astype(BF)
    for start in range(0, depth, sub):
        rows = w[start : start + sub].reshape(2 * sub, units)
        moved = dot(order, rows).astype(BF)
        here = slice(start, start + sub)
        part = block // 2 if paired else block
        for j in range(units // part):
            cols = slice(j * part, (j + 1) * part)
            if paired:
                out[j, here, :part] = moved[:sub, cols]
                out[j, here, part:] = moved[sub:, cols]
            else:
                out[j, here, :] = moved[:sub, cols]
                out[blocks // 2 + j, here, :] = moved[sub:, cols]


def split_gate_up(w, block, paired, part=0, parts=1, depth=512, sub=128):
    _, _, units = w.shape
    width = w.shape[0] // parts
    first = part * (width // depth)
    blocks = 2 * units // block
    return pl.pallas_call(
        functools.partial(split_kernel, sub=sub, paired=paired),
        grid=(width // depth,),
        in_specs=[pl.BlockSpec((depth, 2, units), lambda i: (first + i, 0, 0))],
        out_specs=pl.BlockSpec((blocks, depth, block), lambda i: (0, i, 0)),
        out_shape=pltpu.HBM((blocks, width, block), BF),
        compiler_params=params(20),
        name="split",
    )(far(w))


def unfold_kernel(me, arrived, w_left, w_right, x_out, part_out):
    @pl.when(pl.program_id(0) == 0)
    def _():
        half = arrived.shape[1]
        rows = arrived.shape[0] // 2
        row, col = iota((rows, 2 * rows), 0), iota((rows, 2 * rows), 1)
        first = row // CAP * (2 * CAP) + row % CAP
        for h in range(2):
            pick = jnp.where(col == first + h * CAP, 1.0, 0.0).astype(BF)
            x_out[:, h * half : (h + 1) * half] = dot(pick, arrived[...]).astype(BF)

    part_out[...] = halves_dot(x_out, w_left, w_right).astype(part_out.dtype)


def halves_dot(x, w_left, w_right):
    half = w_left.shape[1]
    return dot(x[:, :half], w_left[0]) + dot(x[:, half:], w_right[0])


def half_block(j, mine, blocks):
    return j // blocks * 2 * blocks + mine * blocks + j % blocks


def send_half(arrived, w, me):
    lanes, half = arrived.shape
    rows, block = lanes // 2, w[0].shape[2]
    blocks = w[0].shape[0] // 4
    units = 2 * blocks * block
    return pl.pallas_call(
        unfold_kernel,
        grid_spec=pltpu.PrefetchScalarGridSpec(
            num_scalar_prefetch=1,
            grid=(2 * blocks,),
            in_specs=[
                pl.BlockSpec((lanes, half), lambda j, me: (0, 0)),
            ]
            + [
                pl.BlockSpec(
                    (1, half, block), lambda j, me: (half_block(j, 1 - me[0], blocks), 0, 0)
                )
            ]
            * 2,
            out_specs=(
                pl.BlockSpec((rows, 2 * half), lambda j, me: (0, 0)),
                pl.BlockSpec((rows, block), lambda j, me: (0, j)),
            ),
        ),
        out_shape=(
            jax.ShapeDtypeStruct((rows, 2 * half), BF),
            jax.ShapeDtypeStruct((rows, units), BF),
        ),
        compiler_params=params(),
        name="send_half",
    )(me, arrived, far(w[0]), far(w[1]))


def keep_kernel(me, x, w_left, w_right, out):
    out[...] = halves_dot(x, w_left, w_right)


def keep_half(x, w, me):
    rows, width = x.shape
    block = w[0].shape[2]
    blocks = w[0].shape[0] // 4
    units = 2 * blocks * block
    return pl.pallas_call(
        keep_kernel,
        grid_spec=pltpu.PrefetchScalarGridSpec(
            num_scalar_prefetch=1,
            grid=(2 * blocks,),
            in_specs=[
                pl.BlockSpec((rows, width), lambda j, me: (0, 0)),
            ]
            + [
                pl.BlockSpec(
                    (1, width // 2, block), lambda j, me: (half_block(j, me[0], blocks), 0, 0)
                )
            ]
            * 2,
            out_specs=pl.BlockSpec((rows, block), lambda j, me: (0, j)),
        ),
        out_shape=jax.ShapeDtypeStruct((rows, units), F32),
        compiler_params=params(),
        name="keep_half",
    )(me, x, far(w[0]), far(w[1]))


def act_kernel(kept, came, out):
    units = out.shape[1]
    pre = kept[...] + came[...].astype(F32)
    out[...] = silu_mul(pre[:, :units], pre[:, units:])


def activate(kept, came):
    rows, units = kept.shape
    return pl.pallas_call(
        act_kernel,
        out_shape=jax.ShapeDtypeStruct((rows, units // 2), BF),
        compiler_params=params(),
        name="activate",
    )(kept, came)


def answer_kernel(me, mine, other, w_mine_l, w_other_l, w_mine_r, w_other_r, out):
    rows = mine.shape[0]
    row, col = iota((2 * rows, rows), 0), iota((2 * rows, rows), 1)
    first = col // CAP * (2 * CAP) + col % CAP
    total = jnp.zeros(out.shape, F32)
    for h, (wm, wo) in enumerate(((w_mine_l, w_other_l), (w_mine_r, w_other_r))):
        answer = (dot(mine[...], wm[...]) + dot(other[...], wo[...])).astype(BF)
        total += dot(jnp.where(row == first + h * CAP, 1.0, 0.0).astype(BF), answer)
    out[...] = total.astype(BF)


def answers(mine, other, w, me, block=512):
    rows, units = mine.shape
    width = w.shape[1]
    blocks = width // 2 // block

    def part(side, h):
        return pl.BlockSpec(
            (units, block),
            lambda n, me: ((me[0] if side else 1 - me[0]), h * blocks + n),
        )

    whole = pl.BlockSpec((rows, units), lambda n, me: (0, 0))
    return pl.pallas_call(
        answer_kernel,
        grid_spec=pltpu.PrefetchScalarGridSpec(
            num_scalar_prefetch=1,
            grid=(blocks,),
            in_specs=[whole, whole, part(1, 0), part(0, 0), part(1, 1), part(0, 1)],
            out_specs=pl.BlockSpec((2 * rows, block), lambda n, me: (0, n)),
        ),
        out_shape=pltpu.HBM((2 * rows, width // 2), BF),
        compiler_params=params(),
        name="answers",
    )(me, mine, other, *(far(w),) * 4)


def shared_kernel(*refs):
    *pieces, w, sent, kept = refs
    start = 0
    for piece in pieces:
        rows = slice(start, start + piece.shape[0])
        start += piece.shape[0]
        pre = dot(piece[...], w[0])
        sent[rows, :] = pre.astype(BF)
        kept[rows, :] = pre


def shared_in_part(pieces, w):
    rows = sum(piece.shape[0] for piece in pieces)
    blocks, width, block = w.shape
    part = pl.BlockSpec((rows, block), lambda j: (0, j))
    return pl.pallas_call(
        shared_kernel,
        grid=(blocks,),
        in_specs=[pl.BlockSpec(memory_space=pltpu.VMEM)] * len(pieces)
        + [pl.BlockSpec((1, width, block), lambda j: (j, 0, 0))],
        out_specs=(part, part),
        out_shape=(
            jax.ShapeDtypeStruct((rows, blocks * block), BF),
            pltpu.HBM((rows, blocks * block), F32),
        ),
        compiler_params=params(),
        name="shared_in",
    )(*pieces, far(w))


def paired_act(kept, came, block=256):
    pre = kept + came.astype(F32)
    half = block // 2
    return jnp.concatenate(
        [
            silu_mul(pre[:, j : j + half], pre[:, j + half : j + block])
            for j in range(0, pre.shape[1], block)
        ],
        axis=1,
    )


def out_kernel(kept, came, w, act_out, *outs):
    act = paired_act(kept[...], came[...])
    act_out[...] = act
    rows = outs[0].shape[0]
    first = act.shape[0] - rows * len(outs)
    total = dot(act[first:, :], w[...])
    for i, out in enumerate(outs):
        out[...] = total[i * rows : (i + 1) * rows].astype(BF)


def shared_out_part(kept, came, w, count, rows):
    units, width = w.shape
    return pl.pallas_call(
        out_kernel,
        in_specs=[pl.BlockSpec(memory_space=pltpu.VMEM)] * 3,
        out_shape=(jax.ShapeDtypeStruct((kept.shape[0], units), BF),)
        + (jax.ShapeDtypeStruct((rows, width), BF),) * count,
        compiler_params=params(),
        name="shared_out",
    )(kept, came, w)


def base_kernel(act, w, a, b, c, out):
    total = dot(act[...], w[...])
    out[...] = total + a[...].astype(F32) + b[...].astype(F32) + c[...].astype(F32)


def shared_sum(act, w, a, b, c, block=768):
    units, width = w.shape
    tokens = a.shape[0]
    part = pl.BlockSpec((tokens, block), lambda j: (0, j))
    return pl.pallas_call(
        base_kernel,
        grid=(width // block,),
        in_specs=[
            pl.BlockSpec((tokens, units), lambda j: (0, 0)),
            pl.BlockSpec((units, block), lambda j: (0, j)),
        ]
        + [part] * 3,
        out_specs=part,
        out_shape=pltpu.HBM((tokens, width), F32),
        compiler_params=params(),
        name="shared_sum",
    )(*(far(x) for x in (act, w, a, b, c)))


def turn_kernel(high, low, out):
    lanes, tokens = high.shape
    side = iota((tokens, lanes), 1) % (2 * CAP) // CAP
    for i, gates in enumerate((high, low)):
        turned = gates[...].astype(F32).T
        for h in range(2):
            out[h, i * tokens : (i + 1) * tokens, :] = jnp.where(side == h, turned, 0.0).astype(BF)


def turn_gates(high, low):
    lanes, tokens = high.shape
    return pl.pallas_call(
        turn_kernel,
        grid=(1,),
        out_shape=pltpu.HBM((2, 2 * tokens, lanes), BF),
        compiler_params=params(),
        name="turn_gates",
    )(high, low)


def mix_kernel(gates, back, base, out):
    tokens = out.shape[0]
    both = dot(gates[0], back[...])
    out[...] = (base[...] + both[:tokens] + both[tokens:]).astype(BF)


def mix(gates, back, base, block=768):
    _, both, lanes = gates.shape
    tokens, width = base.shape
    blocks = width // 2 // block
    part = pl.BlockSpec((tokens, block), lambda j: (0, j))
    return pl.pallas_call(
        mix_kernel,
        grid=(2 * blocks,),
        in_specs=[
            pl.BlockSpec((1, both, lanes), lambda j: (j // blocks, 0, 0)),
            pl.BlockSpec((lanes, block), lambda j: (0, j % blocks)),
            part,
        ],
        out_specs=part,
        out_shape=jax.ShapeDtypeStruct((tokens, width), BF),
        compiler_params=params(),
        name="mix",
    )(far(gates), back, far(base))


def shift(array, axis, by):
    size = lax.axis_size(axis)
    return lax.ppermute(array, axis, [(i, (i + by) % size) for i in range(size)])


def exchange(rows):
    return lax.all_to_all(rows, ("dp", "expert"), split_axis=0, concat_axis=0, tiled=True)


def shards(
    hidden, expert_ids, gate_fixed, slot_expert, expert_in, expert_out, shared_in, shared_out
):
    tokens, width = hidden.shape
    slots = slot_expert.shape[0]
    half = width // 2
    me = lax.axis_index("tensor").astype(jnp.int32)[None]

    prev = shift(hidden, "dp", 1)
    nxt = shift(hidden, "dp", -1)
    send_rows, high, low = route(expert_ids, gate_fixed, slot_expert, hidden)
    arrived = exchange(send_rows.reshape(slots, 2 * CAP, half))
    arrived = arrived.reshape(-1, half)
    w_in = []
    for part in range(2):
        w_in.append(split_gate_up(expert_in[0], 256, False, part, 2))
    w_shared = split_gate_up(shared_in, 256, True, depth=1024)
    n_sent, n_kept = shared_in_part((hidden, prev, nxt), w_shared)
    n_came = shift(n_sent, "tensor", 1)
    opposite = shift(hidden, "dp", 2)

    x, sent = send_half(arrived, w_in, me)
    came = shift(sent, "tensor", 1)
    kept = keep_half(x, w_in, me)
    own_act, down, up = shared_out_part(n_kept, n_came, shared_out, 2, tokens)
    from_prev = shift(up, "dp", 1)
    from_next = shift(down, "dp", -1)
    f_sent, f_kept = shared_in_part((opposite,), w_shared)
    f_came = shift(f_sent, "tensor", 1)

    act = activate(kept, came)
    act_other = shift(act, "tensor", 1)
    _, far_part = shared_out_part(f_kept, f_came, shared_out, 1, tokens)
    from_far = shift(far_part, "dp", 2)

    rows = answers(act, act_other, expert_out[0], me)
    back = exchange(rows.reshape(slots, 2 * CAP, half))
    back = back.reshape(-1, half)
    gates = turn_gates(high, low)
    base = shared_sum(own_act, shared_out, from_prev, from_next, from_far)
    return mix(gates, back, base)


def solution(mesh):
    in_specs = (
        P(("dp", "expert"), "tensor"),
        P(("dp", "expert"), None),
        P(("dp", "expert"), None),
        P(),
        P(("dp", "expert"), "tensor", None, None),
        P(("dp", "expert"), None, "tensor"),
        P("tensor", None, "dp"),
        P("dp", "tensor"),
    )
    out_specs = P(("dp", "expert"), "tensor")
    return jax.shard_map(shards, mesh=mesh, in_specs=in_specs, out_specs=out_specs, check_vma=False)
```

```python
import functools

import jax
import jax.numpy as jnp
from jax import lax
from jax.experimental import pallas as pl
from jax.experimental.pallas import tpu as pltpu
from jax.sharding import PartitionSpec as P


CAP = 4
BF = jnp.bfloat16
F32 = jnp.float32


def params(mib=20):
    return pltpu.CompilerParams(vmem_limit_bytes=mib * 2**20)


def far(array):
    return pltpu.with_memory_space_constraint(array, pltpu.HBM)


def dot(a, b):
    return jnp.dot(a, b, preferred_element_type=F32)


def iota(shape, dim):
    return lax.broadcasted_iota(jnp.int32, shape, dim)


def silu_mul(gate, up):
    return (jax.nn.silu(gate) * up).astype(BF)


def served_lanes(ids, held_row):
    slots = held_row.shape[1]
    lanes = slots * 2 * CAP
    tokens = ids.shape[1]
    col, slot = iota((lanes, slots), 1), iota((lanes, slots), 0) >> 3
    held_all = jnp.broadcast_to(held_row[...], (lanes, slots))
    held = jnp.max(jnp.where(col == slot, held_all, -1), axis=1, keepdims=True)
    twin = (held_all == held) & (col < slot)
    spare = jnp.max(jnp.where(twin, CAP, 0), axis=1, keepdims=True)
    named = jnp.zeros((lanes, tokens), F32)
    for k in range(ids.shape[0]):
        named = jnp.where(ids[k : k + 1, :] == held, 1.0, named)
    earlier = iota((tokens, tokens), 0) < iota((tokens, tokens), 1)
    rank = dot(named.astype(BF), jnp.where(earlier, 1.0, 0.0).astype(BF))
    row = iota((lanes, 1), 0)
    place = (spare + (row & (CAP - 1))).astype(F32)
    served = (named > 0.5) & (rank == place)
    return served, held, (row & CAP) == 0


def route_kernel(ids, held_row, left, right, rows_out, pick):
    @pl.when(pl.program_id(0) == 0)
    def _():
        served, _, is_left = served_lanes(ids, held_row)
        one = jnp.where(served, 1.0, 0.0)
        pick[0] = jnp.where(is_left, one, 0.0).astype(BF)
        pick[1] = jnp.where(is_left, 0.0, one).astype(BF)

    rows_out[...] = (dot(pick[0], left[...]) + dot(pick[1], right[...])).astype(BF)


def whole_of(array):
    return pl.BlockSpec(array.shape, lambda *_: (0,) * array.ndim)


def route(ids, slot_expert, hidden, block=768):
    slots = slot_expert.shape[0]
    lanes = slots * 2 * CAP
    tokens, width = hidden.shape
    half = width // 2
    blocks = half // block
    ids, held = ids.T, slot_expert[None]
    return pl.pallas_call(
        route_kernel,
        grid=(blocks,),
        in_specs=[
            whole_of(ids),
            whole_of(held),
            pl.BlockSpec((tokens, block), lambda j: (0, j)),
            pl.BlockSpec((tokens, block), lambda j: (0, blocks + j)),
        ],
        out_specs=pl.BlockSpec((lanes, block), lambda j: (0, j)),
        out_shape=pltpu.HBM((lanes, half), BF),
        scratch_shapes=[pltpu.VMEM((2, lanes, tokens), BF)],
        compiler_params=params(16),
        name="route",
    )(*(far(x) for x in (ids, held, hidden, hidden)))


def gates_kernel(ids, gates, held_row, out):
    served, held, is_left = served_lanes(ids, held_row)
    tokens = ids.shape[1]
    gate = jnp.zeros(served.shape, jnp.int32)
    for k in range(ids.shape[0]):
        gate = gate + jnp.where(ids[k : k + 1, :] == held, gates[k : k + 1, :], 0)
    gate = jnp.where(served, gate, 0)
    high = (gate >> 8).astype(F32) * 2.0**-8
    low = (gate & 255).astype(F32) * 2.0**-16
    for i, part in enumerate((high, low)):
        rows = slice(i * tokens, (i + 1) * tokens)
        out[0, rows, :] = jnp.where(is_left, part, 0.0).T.astype(BF)
        out[1, rows, :] = jnp.where(is_left, 0.0, part).T.astype(BF)


def combine_gates(ids, gates, slot_expert):
    lanes = slot_expert.shape[0] * 2 * CAP
    operands = ids.T, gates.T, slot_expert[None]
    shape = (2, 2 * ids.shape[0], lanes)
    return pl.pallas_call(
        gates_kernel,
        grid=(1,),
        in_specs=[whole_of(x) for x in operands],
        out_specs=pl.BlockSpec(shape, lambda j: (0, 0, 0)),
        out_shape=pltpu.HBM(shape, BF),
        compiler_params=params(16),
        name="combine_gates",
    )(*(far(x) for x in operands))


def split_kernel(w, w_shared, out, out_shared, *, sub):
    row, col = iota((2 * sub, 2 * sub), 0), iota((2 * sub, 2 * sub), 1)
    source = jnp.where(row < sub, 2 * row, 2 * (row - sub) + 1)
    order = jnp.where(col == source, 1.0, 0.0).astype(BF)
    block, part = out.shape[2], out_shared.shape[2] // 2
    for start in range(0, w.shape[0], sub):
        here = slice(start, start + sub)
        moved = dot(order, w[here].reshape(2 * sub, w.shape[2])).astype(BF)
        for j in range(2):
            cols = slice(j * block, (j + 1) * block)
            out[j, here, :] = moved[:sub, cols]
            out[2 + j, here, :] = moved[sub:, cols]
        moved = dot(order, w_shared[here].reshape(2 * sub, w_shared.shape[2])).astype(BF)
        for j in range(2):
            cols = slice(j * part, (j + 1) * part)
            out_shared[j, here, :part] = moved[:sub, cols]
            out_shared[j, here, part:] = moved[sub:, cols]


def split_gate_up(w, w_shared, depth=768, sub=128):
    width, _, units = w.shape
    shared_units = w_shared.shape[2]

    def taken(columns):
        return pl.BlockSpec((depth, 2, columns), lambda i: (i, 0, 0))

    def given(blocks, block):
        return pl.BlockSpec((blocks, depth, block), lambda i: (0, i, 0))

    return pl.pallas_call(
        functools.partial(split_kernel, sub=sub),
        grid=(width // depth,),
        in_specs=[taken(units), taken(shared_units)],
        out_specs=(given(4, units // 2), given(2, shared_units)),
        out_shape=(
            pltpu.HBM((4, width, units // 2), BF),
            pltpu.HBM((2, width, shared_units), BF),
        ),
        compiler_params=params(24),
        name="split",
    )(far(w), far(w_shared))


def fetch(w, held, sems, side):
    copies = []
    cut = w.shape[1] // 2
    for j in range(2):
        for k in range(2):
            rows = slice(k * cut, (k + 1) * cut)
            copies.append(
                pltpu.make_async_copy(
                    w.at[2 * j + side, rows], held.at[j, rows], sems.at[2 * j + k]
                )
            )
            copies[-1].start()
    return copies


def multiply(x, held, copies, out):
    cut, block = held.shape[1] // 2, held.shape[2]
    for j in range(2):
        total = None
        for k in range(2):
            copies[2 * j + k].wait()
            rows = slice(k * cut, (k + 1) * cut)
            part = dot(x[:, rows], held[j, rows])
            total = part if total is None else total + part
        out[:, j * block : (j + 1) * block] = total.astype(out.dtype)


def send_kernel(me, arrived, w, x_out, out, held, sems):
    copies = fetch(w, held, sems, 1 - me[0])
    half = arrived.shape[1]
    rows = arrived.shape[0] // 2
    row, col = iota((rows, 2 * rows), 0), iota((rows, 2 * rows), 1)
    first = ((row >> 2) << 3) + (row & 3)
    for h in range(2):
        pick = jnp.where(col == first + h * CAP, 1.0, 0.0).astype(BF)
        x_out[:, h * half : (h + 1) * half] = dot(pick, arrived[...]).astype(BF)
    multiply(x_out, held, copies, out)


def weight_scratch(w):
    return [pltpu.VMEM((2, *w.shape[1:]), BF), pltpu.SemaphoreType.DMA((4,))]


def send_half(arrived, w, me):
    lanes, half = arrived.shape
    rows, units = lanes // 2, 2 * w.shape[2]
    near = pl.BlockSpec(memory_space=pltpu.VMEM)
    return pl.pallas_call(
        send_kernel,
        in_specs=[pl.BlockSpec(memory_space=pltpu.SMEM), near, pl.BlockSpec(memory_space=pl.ANY)],
        out_shape=(
            jax.ShapeDtypeStruct((rows, 2 * half), BF),
            jax.ShapeDtypeStruct((rows, units), BF),
        ),
        scratch_shapes=weight_scratch(w),
        compiler_params=params(),
        name="send_half",
    )(me, arrived, far(w))


def keep_kernel(me, x, w, out, held, sems):
    multiply(x, held, fetch(w, held, sems, me[0]), out)


def keep_half(x, w, me):
    near = pl.BlockSpec(memory_space=pltpu.VMEM)
    return pl.pallas_call(
        keep_kernel,
        in_specs=[pl.BlockSpec(memory_space=pltpu.SMEM), near, pl.BlockSpec(memory_space=pl.ANY)],
        out_shape=jax.ShapeDtypeStruct((x.shape[0], 2 * w.shape[2]), F32),
        scratch_shapes=weight_scratch(w),
        compiler_params=params(),
        name="keep_half",
    )(me, x, far(w))


def act_kernel(kept, came, out):
    units = out.shape[1]
    pre = kept[...] + came[...].astype(F32)
    out[...] = silu_mul(pre[:, :units], pre[:, units:])


def activate(kept, came):
    rows, units = kept.shape
    return pl.pallas_call(
        act_kernel,
        out_shape=jax.ShapeDtypeStruct((rows, units // 2), BF),
        compiler_params=params(),
        name="activate",
    )(kept, came)


def answer_kernel(me, mine, other, w, out, *, block):
    rows, units = mine.shape
    half = out.shape[1]
    row, col = iota((2 * rows, rows), 0), iota((2 * rows, rows), 1)
    first = ((col >> 2) << 3) + (col & 3)
    place = [jnp.where(row == first + h * CAP, 1.0, 0.0).astype(BF) for h in range(2)]
    at_mine = pl.ds(pl.multiple_of(me[0] * units, units), units)
    at_other = pl.ds(pl.multiple_of((1 - me[0]) * units, units), units)

    def answer(start):
        cols = slice(start, start + block)
        return (dot(mine[...], w[at_mine, cols]) + dot(other[...], w[at_other, cols])).astype(BF)

    for start in range(0, half, block):
        total = dot(place[0], answer(start)) + dot(place[1], answer(half + start))
        out[:, start : start + block] = total.astype(BF)


def answers(mine, other, w, me, block=768):
    rows, _ = mine.shape
    near = pl.BlockSpec(memory_space=pltpu.VMEM)
    return pl.pallas_call(
        functools.partial(answer_kernel, block=block),
        in_specs=[pl.BlockSpec(memory_space=pltpu.SMEM)] + [near] * 3,
        out_shape=jax.ShapeDtypeStruct((2 * rows, w.shape[1] // 2), BF),
        compiler_params=params(),
        name="answers",
    )(me, mine, other, w)


def shared_kernel(*refs, count, ahead):
    pieces, w, sent, kept = refs[:count], *refs[count : count + 3]
    pre = dot(jnp.concatenate([piece[...] for piece in pieces], axis=0), w[0])
    sent[...] = pre.astype(BF)
    kept[...] = pre
    if ahead:

        @pl.when(pl.program_id(0) == 0)
        def _():
            up, down = refs[count + 3 :]
            rows = up.shape[0]
            up[...] = pieces[1][:rows, :]
            down[...] = pieces[2][rows:, :]


def shared_in_part(pieces, w, ahead):
    rows = sum(piece.shape[0] for piece in pieces)
    blocks, width, block = w.shape
    part = pl.BlockSpec((rows, block), lambda j: (0, j))
    out_specs = [part, part]
    out_shape = [
        jax.ShapeDtypeStruct((rows, blocks * block), BF),
        pltpu.HBM((rows, blocks * block), F32),
    ]
    if ahead:
        shape = (pieces[0].shape[0] // 2, width)
        out_specs += [pl.BlockSpec(shape, lambda j: (0, 0))] * 2
        out_shape += [jax.ShapeDtypeStruct(shape, BF)] * 2
    return pl.pallas_call(
        functools.partial(shared_kernel, count=len(pieces), ahead=ahead),
        grid=(blocks,),
        in_specs=[pl.BlockSpec(memory_space=pltpu.VMEM)] * len(pieces)
        + [pl.BlockSpec((1, width, block), lambda j: (j, 0, 0))],
        out_specs=tuple(out_specs),
        out_shape=tuple(out_shape),
        compiler_params=params(),
        name="shared_in",
    )(*pieces, far(w))


def paired_act(kept, came, block=256):
    pre = kept + came.astype(F32)
    half = block // 2
    return jnp.concatenate(
        [
            silu_mul(pre[:, j : j + half], pre[:, j + half : j + block])
            for j in range(0, pre.shape[1], block)
        ],
        axis=1,
    )


def out_kernel(kept, came, w, act_out, *outs):
    act = paired_act(kept[...], came[...])
    act_out[...] = act
    rows = outs[0].shape[0]
    first = act.shape[0] - rows * len(outs)
    total = dot(act[first:, :], w[...])
    for i, out in enumerate(outs):
        out[...] = total[i * rows : (i + 1) * rows].astype(BF)


def shared_out_part(kept, came, w, count, rows):
    units, width = w.shape
    return pl.pallas_call(
        out_kernel,
        in_specs=[pl.BlockSpec(memory_space=pltpu.VMEM)] * 3,
        out_shape=(jax.ShapeDtypeStruct((kept.shape[0], units), BF),)
        + (jax.ShapeDtypeStruct((rows, width), BF),) * count,
        compiler_params=params(),
        name="shared_out",
    )(kept, came, w)


def base_kernel(act, w, out):
    out[...] = dot(act[...], w[...])


def own_sum(act, w, tokens, block=1536):
    units, width = w.shape
    return pl.pallas_call(
        base_kernel,
        grid=(width // block,),
        in_specs=[
            pl.BlockSpec((tokens, units), lambda j: (0, 0)),
            pl.BlockSpec((units, block), lambda j: (0, j)),
        ],
        out_specs=pl.BlockSpec((tokens, block), lambda j: (0, j)),
        out_shape=pltpu.HBM((tokens, width), F32),
        compiler_params=params(),
        name="own_sum",
    )(far(act), far(w))


def mix_kernel(gates, back, base, a, b, c, out):
    tokens = out.shape[0]
    total = base[...] + a[...].astype(F32) + b[...].astype(F32) + c[...].astype(F32)
    both = dot(gates[0], back[...])
    out[...] = (total + both[:tokens] + both[tokens:]).astype(BF)


def mix(gates, back, base, came, block=1536):
    _, both, lanes = gates.shape
    tokens, width = base.shape
    blocks = width // 2 // block
    part = pl.BlockSpec((tokens, block), lambda j: (0, j))
    return pl.pallas_call(
        mix_kernel,
        grid=(2 * blocks,),
        in_specs=[
            pl.BlockSpec((1, both, lanes), lambda j: (j // blocks, 0, 0)),
            pl.BlockSpec((lanes, block), lambda j: (0, j % blocks)),
        ]
        + [part] * 4,
        out_specs=part,
        out_shape=jax.ShapeDtypeStruct((tokens, width), BF),
        compiler_params=params(),
        name="mix",
    )(far(gates), back, far(base), *(far(x) for x in came))


def shift(array, axis, by):
    size = lax.axis_size(axis)
    return lax.ppermute(array, axis, [(i, (i + by) % size) for i in range(size)])


def exchange(rows):
    return lax.all_to_all(rows, ("dp", "expert"), split_axis=0, concat_axis=0, tiled=True)


def shards(
    hidden, expert_ids, gate_fixed, slot_expert, expert_in, expert_out, shared_in, shared_out
):
    tokens, width = hidden.shape
    slots = slot_expert.shape[0]
    half = width // 2
    me = lax.axis_index("tensor").astype(jnp.int32)[None]

    prev = shift(hidden, "dp", 1)
    nxt = shift(hidden, "dp", -1)
    send_rows = route(expert_ids, slot_expert, hidden)
    arrived = exchange(send_rows.reshape(slots, 2 * CAP, half))
    arrived = arrived.reshape(-1, half)
    w_in, w_shared = split_gate_up(expert_in[0], shared_in)
    n_sent, n_kept, ahead, behind = shared_in_part((hidden, prev, nxt), w_shared, True)
    n_came = shift(n_sent, "tensor", 1)
    far_a = shift(ahead, "dp", 1)
    far_b = shift(behind, "dp", -1)

    x, sent = send_half(arrived, w_in, me)
    came = shift(sent, "tensor", 1)
    kept = keep_half(x, w_in, me)
    own_act, down, up = shared_out_part(n_kept, n_came, shared_out, 2, tokens)
    from_prev = shift(up, "dp", 1)
    from_next = shift(down, "dp", -1)
    f_sent, f_kept = shared_in_part((far_a, far_b), w_shared, False)
    f_came = shift(f_sent, "tensor", 1)

    act = activate(kept, came)
    act_other = shift(act, "tensor", 1)
    _, far_part = shared_out_part(f_kept, f_came, shared_out, 1, tokens)
    from_far = shift(far_part, "dp", 2)

    rows = answers(act, act_other, expert_out[0], me)
    back = exchange(rows.reshape(slots, 2 * CAP, half))
    back = back.reshape(-1, half)
    gates = combine_gates(expert_ids, gate_fixed, slot_expert)
    base = own_sum(own_act, shared_out, tokens)
    return mix(gates, back, base, (from_prev, from_next, from_far))


def solution(mesh):
    in_specs = (
        P(("dp", "expert"), "tensor"),
        P(("dp", "expert"), None),
        P(("dp", "expert"), None),
        P(),
        P(("dp", "expert"), "tensor", None, None),
        P(("dp", "expert"), None, "tensor"),
        P("tensor", None, "dp"),
        P("dp", "tensor"),
    )
    out_specs = P(("dp", "expert"), "tensor")
    return jax.shard_map(shards, mesh=mesh, in_specs=in_specs, out_specs=out_specs, check_vma=False)
```

```python
import functools

import jax
import jax.numpy as jnp
from jax import lax
from jax.experimental import pallas as pl
from jax.experimental.pallas import tpu as pltpu
from jax.sharding import PartitionSpec as P


CAP = 4
BF = jnp.bfloat16
F32 = jnp.float32


def params(mib=20):
    return pltpu.CompilerParams(vmem_limit_bytes=mib * 2**20)


def far(array):
    return pltpu.with_memory_space_constraint(array, pltpu.HBM)


def dot(a, b):
    return jnp.dot(a, b, preferred_element_type=F32)


def iota(shape, dim):
    return lax.broadcasted_iota(jnp.int32, shape, dim)


def silu_mul(gate, up):
    return (jax.nn.silu(gate) * up).astype(BF)


def served_lanes(ids, held_row):
    slots = held_row.shape[1]
    lanes = slots * 2 * CAP
    tokens = ids.shape[1]
    col, slot = iota((lanes, slots), 1), iota((lanes, slots), 0) >> 3
    held_all = jnp.broadcast_to(held_row[...], (lanes, slots))
    held = jnp.max(jnp.where(col == slot, held_all, -1), axis=1, keepdims=True)
    twin = (held_all == held) & (col < slot)
    spare = jnp.max(jnp.where(twin, CAP, 0), axis=1, keepdims=True)
    named = jnp.zeros((lanes, tokens), F32)
    for k in range(ids.shape[0]):
        named = jnp.where(ids[k : k + 1, :] == held, 1.0, named)
    earlier = iota((tokens, tokens), 0) < iota((tokens, tokens), 1)
    rank = dot(named.astype(BF), jnp.where(earlier, 1.0, 0.0).astype(BF))
    row = iota((lanes, 1), 0)
    place = (spare + (row & (CAP - 1))).astype(F32)
    served = (named > 0.5) & (rank == place)
    return served, held, (row & CAP) == 0


def route_kernel(ids, held_row, left, right, rows_out, pick):
    @pl.when(pl.program_id(0) == 0)
    def _():
        served, _, is_left = served_lanes(ids, held_row)
        one = jnp.where(served, 1.0, 0.0)
        pick[0] = jnp.where(is_left, one, 0.0).astype(BF)
        pick[1] = jnp.where(is_left, 0.0, one).astype(BF)

    rows_out[...] = (dot(pick[0], left[...]) + dot(pick[1], right[...])).astype(BF)


def whole_of(array):
    return pl.BlockSpec(array.shape, lambda *_: (0,) * array.ndim)


def route(ids, slot_expert, hidden, block=768):
    slots = slot_expert.shape[0]
    lanes = slots * 2 * CAP
    tokens, width = hidden.shape
    half = width // 2
    blocks = half // block
    ids, held = ids.T, slot_expert[None]
    return pl.pallas_call(
        route_kernel,
        grid=(blocks,),
        in_specs=[
            whole_of(ids),
            whole_of(held),
            pl.BlockSpec((tokens, block), lambda j: (0, j)),
            pl.BlockSpec((tokens, block), lambda j: (0, blocks + j)),
        ],
        out_specs=pl.BlockSpec((lanes, block), lambda j: (0, j)),
        out_shape=pltpu.HBM((lanes, half), BF),
        scratch_shapes=[pltpu.VMEM((2, lanes, tokens), BF)],
        compiler_params=params(16),
        name="route",
    )(*(far(x) for x in (ids, held, hidden, hidden)))


def gates_kernel(ids, gates, held_row, out):
    served, held, is_left = served_lanes(ids, held_row)
    tokens = ids.shape[1]
    gate = jnp.zeros(served.shape, jnp.int32)
    for k in range(ids.shape[0]):
        gate = gate + jnp.where(ids[k : k + 1, :] == held, gates[k : k + 1, :], 0)
    gate = jnp.where(served, gate, 0)
    high = (gate >> 8).astype(F32) * 2.0**-8
    low = (gate & 255).astype(F32) * 2.0**-16
    for i, part in enumerate((high, low)):
        rows = slice(i * tokens, (i + 1) * tokens)
        out[0, rows, :] = jnp.where(is_left, part, 0.0).T.astype(BF)
        out[1, rows, :] = jnp.where(is_left, 0.0, part).T.astype(BF)


def combine_gates(ids, gates, slot_expert):
    lanes = slot_expert.shape[0] * 2 * CAP
    operands = ids.T, gates.T, slot_expert[None]
    shape = (2, 2 * ids.shape[0], lanes)
    return pl.pallas_call(
        gates_kernel,
        grid=(1,),
        in_specs=[whole_of(x) for x in operands],
        out_specs=pl.BlockSpec(shape, lambda j: (0, 0, 0)),
        out_shape=pltpu.HBM(shape, BF),
        compiler_params=params(16),
        name="combine_gates",
    )(*(far(x) for x in operands))


def split_kernel(w, w_shared, out, out_shared, *, sub):
    row, col = iota((2 * sub, 2 * sub), 0), iota((2 * sub, 2 * sub), 1)
    source = jnp.where(row < sub, 2 * row, 2 * (row - sub) + 1)
    order = jnp.where(col == source, 1.0, 0.0).astype(BF)
    block, part = out.shape[2], out_shared.shape[2] // 2
    for start in range(0, w.shape[0], sub):
        here = slice(start, start + sub)
        moved = dot(order, w[here].reshape(2 * sub, w.shape[2])).astype(BF)
        for j in range(2):
            cols = slice(j * block, (j + 1) * block)
            out[j, here, :] = moved[:sub, cols]
            out[2 + j, here, :] = moved[sub:, cols]
        moved = dot(order, w_shared[here].reshape(2 * sub, w_shared.shape[2])).astype(BF)
        for j in range(2):
            cols = slice(j * part, (j + 1) * part)
            out_shared[j, here, :part] = moved[:sub, cols]
            out_shared[j, here, part:] = moved[sub:, cols]


def split_gate_up(w, w_shared, depth=768, sub=128):
    width, _, units = w.shape
    shared_units = w_shared.shape[2]

    def taken(columns):
        return pl.BlockSpec((depth, 2, columns), lambda i: (i, 0, 0))

    def given(blocks, block):
        return pl.BlockSpec((blocks, depth, block), lambda i: (0, i, 0))

    return pl.pallas_call(
        functools.partial(split_kernel, sub=sub),
        grid=(width // depth,),
        in_specs=[taken(units), taken(shared_units)],
        out_specs=(given(4, units // 2), given(2, shared_units)),
        out_shape=(
            pltpu.HBM((4, width, units // 2), BF),
            pltpu.HBM((2, width, shared_units), BF),
        ),
        compiler_params=params(24),
        name="split",
    )(far(w), far(w_shared))


def fetch(w, held, sems, side):
    copies = []
    cut = w.shape[1] // 2
    for j in range(2):
        for k in range(2):
            rows = slice(k * cut, (k + 1) * cut)
            copies.append(
                pltpu.make_async_copy(
                    w.at[2 * j + side, rows], held.at[j, rows], sems.at[2 * j + k]
                )
            )
            copies[-1].start()
    return copies


def multiply(x, held, copies, out):
    cut, block = held.shape[1] // 2, held.shape[2]
    for j in range(2):
        total = None
        for k in range(2):
            copies[2 * j + k].wait()
            rows = slice(k * cut, (k + 1) * cut)
            part = dot(x[:, rows], held[j, rows])
            total = part if total is None else total + part
        out[:, j * block : (j + 1) * block] = total.astype(out.dtype)


def send_kernel(me, arrived, w, x_out, out, held, sems):
    copies = fetch(w, held, sems, 1 - me[0])
    half = arrived.shape[1]
    rows = arrived.shape[0] // 2
    row, col = iota((rows, 2 * rows), 0), iota((rows, 2 * rows), 1)
    first = ((row >> 2) << 3) + (row & 3)
    for h in range(2):
        pick = jnp.where(col == first + h * CAP, 1.0, 0.0).astype(BF)
        x_out[:, h * half : (h + 1) * half] = dot(pick, arrived[...]).astype(BF)
    multiply(x_out, held, copies, out)


def weight_scratch(w):
    return [pltpu.VMEM((2, *w.shape[1:]), BF), pltpu.SemaphoreType.DMA((4,))]


def send_half(arrived, w, me):
    lanes, half = arrived.shape
    rows, units = lanes // 2, 2 * w.shape[2]
    near = pl.BlockSpec(memory_space=pltpu.VMEM)
    return pl.pallas_call(
        send_kernel,
        in_specs=[pl.BlockSpec(memory_space=pltpu.SMEM), near, pl.BlockSpec(memory_space=pl.ANY)],
        out_shape=(
            jax.ShapeDtypeStruct((rows, 2 * half), BF),
            jax.ShapeDtypeStruct((rows, units), BF),
        ),
        scratch_shapes=weight_scratch(w),
        compiler_params=params(),
        name="send_half",
    )(me, arrived, far(w))


def keep_kernel(me, x, w, out, held, sems):
    multiply(x, held, fetch(w, held, sems, me[0]), out)


def keep_half(x, w, me):
    near = pl.BlockSpec(memory_space=pltpu.VMEM)
    return pl.pallas_call(
        keep_kernel,
        in_specs=[pl.BlockSpec(memory_space=pltpu.SMEM), near, pl.BlockSpec(memory_space=pl.ANY)],
        out_shape=jax.ShapeDtypeStruct((x.shape[0], 2 * w.shape[2]), F32),
        scratch_shapes=weight_scratch(w),
        compiler_params=params(),
        name="keep_half",
    )(me, x, far(w))


def act_kernel(kept, came, out):
    units = out.shape[1]
    pre = kept[...] + came[...].astype(F32)
    out[...] = silu_mul(pre[:, :units], pre[:, units:])


def activate(kept, came):
    rows, units = kept.shape
    return pl.pallas_call(
        act_kernel,
        out_shape=jax.ShapeDtypeStruct((rows, units // 2), BF),
        compiler_params=params(),
        name="activate",
    )(kept, came)


def answer_kernel(me, mine, other, w, out, *, block):
    rows, units = mine.shape
    half = out.shape[1]
    row, col = iota((2 * rows, rows), 0), iota((2 * rows, rows), 1)
    first = ((col >> 2) << 3) + (col & 3)
    place = [jnp.where(row == first + h * CAP, 1.0, 0.0).astype(BF) for h in range(2)]
    at_mine = pl.ds(pl.multiple_of(me[0] * units, units), units)
    at_other = pl.ds(pl.multiple_of((1 - me[0]) * units, units), units)

    def answer(start):
        cols = slice(start, start + block)
        return (dot(mine[...], w[at_mine, cols]) + dot(other[...], w[at_other, cols])).astype(BF)

    for start in range(0, half, block):
        total = dot(place[0], answer(start)) + dot(place[1], answer(half + start))
        out[:, start : start + block] = total.astype(BF)


def answers(mine, other, w, me, block=768):
    rows, _ = mine.shape
    near = pl.BlockSpec(memory_space=pltpu.VMEM)
    return pl.pallas_call(
        functools.partial(answer_kernel, block=block),
        in_specs=[pl.BlockSpec(memory_space=pltpu.SMEM)] + [near] * 3,
        out_shape=jax.ShapeDtypeStruct((2 * rows, w.shape[1] // 2), BF),
        compiler_params=params(),
        name="answers",
    )(me, mine, other, w)


def shared_kernel(*refs, count, cuts, ahead):
    pieces, w = refs[:count], refs[count]
    kept, *sent = refs[count + 1 : count + 2 + len(cuts)]
    pre = dot(jnp.concatenate([piece[...] for piece in pieces], axis=0), w[0])
    kept[...] = pre
    start = 0
    for rows, out in zip(cuts, sent):
        out[...] = pre[start : start + rows].astype(BF)
        start += rows
    if ahead:

        @pl.when(pl.program_id(0) == 0)
        def _():
            up, down = refs[-2:]
            rows = up.shape[0]
            up[...] = pieces[0][:rows, :]
            down[...] = pieces[1][rows:, :]


def shared_in_part(pieces, w, cuts, ahead=0):
    rows = sum(piece.shape[0] for piece in pieces)
    blocks, width, block = w.shape

    def part(rows):
        return pl.BlockSpec((rows, block), lambda j: (0, j))

    out_specs = [part(rows)] + [part(cut) for cut in cuts]
    out_shape = [pltpu.HBM((rows, blocks * block), F32)]
    out_shape += [jax.ShapeDtypeStruct((cut, blocks * block), BF) for cut in cuts]
    if ahead:
        out_specs += [pl.BlockSpec((ahead, width), lambda j: (0, 0))] * 2
        out_shape += [jax.ShapeDtypeStruct((ahead, width), BF)] * 2
    return pl.pallas_call(
        functools.partial(shared_kernel, count=len(pieces), cuts=cuts, ahead=ahead),
        grid=(blocks,),
        in_specs=[pl.BlockSpec(memory_space=pltpu.VMEM)] * len(pieces)
        + [pl.BlockSpec((1, width, block), lambda j: (j, 0, 0))],
        out_specs=tuple(out_specs),
        out_shape=tuple(out_shape),
        compiler_params=params(),
        name="shared_in",
    )(*pieces, far(w))


def paired_act(kept, came, block=256):
    pre = kept + came.astype(F32)
    half = block // 2
    return jnp.concatenate(
        [
            silu_mul(pre[:, j : j + half], pre[:, j + half : j + block])
            for j in range(0, pre.shape[1], block)
        ],
        axis=1,
    )


def out_kernel(kept, came, w, *outs):
    rows = outs[0].shape[0]
    total = dot(paired_act(kept[: came.shape[0], :], came[...]), w[...])
    for i, out in enumerate(outs):
        out[...] = total[i * rows : (i + 1) * rows].astype(BF)


def shared_out_part(kept, came, w, count):
    rows, width = came.shape[0] // count, w.shape[1]
    return pl.pallas_call(
        out_kernel,
        in_specs=[pl.BlockSpec(memory_space=pltpu.VMEM)] * 3,
        out_shape=(jax.ShapeDtypeStruct((rows, width), BF),) * count,
        compiler_params=params(),
        name="shared_out",
    )(kept, came, w)


def base_kernel(kept, came, w, out):
    out[...] = dot(paired_act(kept[...], came[...]), w[...])


def own_sum(kept, came, w, block=1536):
    units, width = w.shape
    tokens = came.shape[0]
    return pl.pallas_call(
        base_kernel,
        grid=(width // block,),
        in_specs=[
            pl.BlockSpec((tokens, kept.shape[1]), lambda j: (1, 0)),
            pl.BlockSpec(came.shape, lambda j: (0, 0)),
            pl.BlockSpec((units, block), lambda j: (0, j)),
        ],
        out_specs=pl.BlockSpec((tokens, block), lambda j: (0, j)),
        out_shape=pltpu.HBM((tokens, width), F32),
        compiler_params=params(),
        name="own_sum",
    )(far(kept), far(came), far(w))


def mix_kernel(gates, back, base, a, b, c, out):
    tokens = out.shape[0]
    total = base[...] + a[...].astype(F32) + b[...].astype(F32) + c[...].astype(F32)
    both = dot(gates[0], back[...])
    out[...] = (total + both[:tokens] + both[tokens:]).astype(BF)


def mix(gates, back, base, came, block=1536):
    _, both, lanes = gates.shape
    tokens, width = base.shape
    blocks = width // 2 // block
    part = pl.BlockSpec((tokens, block), lambda j: (0, j))
    return pl.pallas_call(
        mix_kernel,
        grid=(2 * blocks,),
        in_specs=[
            pl.BlockSpec((1, both, lanes), lambda j: (j // blocks, 0, 0)),
            pl.BlockSpec((lanes, block), lambda j: (0, j % blocks)),
        ]
        + [part] * 4,
        out_specs=part,
        out_shape=jax.ShapeDtypeStruct((tokens, width), BF),
        compiler_params=params(),
        name="mix",
    )(far(gates), back, far(base), *(far(x) for x in came))


def shift(array, axis, by):
    size = lax.axis_size(axis)
    return lax.ppermute(array, axis, [(i, (i + by) % size) for i in range(size)])


def exchange(rows):
    return lax.all_to_all(rows, ("dp", "expert"), split_axis=0, concat_axis=0, tiled=True)


def shards(
    hidden, expert_ids, gate_fixed, slot_expert, expert_in, expert_out, shared_in, shared_out
):
    tokens, width = hidden.shape
    slots = slot_expert.shape[0]
    half = width // 2
    me = lax.axis_index("tensor").astype(jnp.int32)[None]

    prev = shift(hidden, "dp", 1)
    nxt = shift(hidden, "dp", -1)
    send_rows = route(expert_ids, slot_expert, hidden)
    arrived = exchange(send_rows.reshape(slots, 2 * CAP, half))
    arrived = arrived.reshape(-1, half)
    w_in, w_shared = split_gate_up(expert_in[0], shared_in)
    n_kept, n_sent, ahead, behind = shared_in_part(
        (prev, nxt), w_shared, (2 * tokens,), tokens // 2
    )
    n_came = shift(n_sent, "tensor", 1)
    far_a = shift(ahead, "dp", 1)
    far_b = shift(behind, "dp", -1)

    x, sent = send_half(arrived, w_in, me)
    came = shift(sent, "tensor", 1)
    kept = keep_half(x, w_in, me)
    down, up = shared_out_part(n_kept, n_came, shared_out, 2)
    from_prev = shift(up, "dp", 1)
    from_next = shift(down, "dp", -1)
    f_kept, f_sent, own_sent = shared_in_part(
        (far_a, far_b, hidden), w_shared, (tokens, tokens)
    )
    f_came = shift(f_sent, "tensor", 1)
    own_came = shift(own_sent, "tensor", 1)

    act = activate(kept, came)
    act_other = shift(act, "tensor", 1)
    (far_part,) = shared_out_part(f_kept, f_came, shared_out, 1)
    from_far = shift(far_part, "dp", 2)

    rows = answers(act, act_other, expert_out[0], me)
    back = exchange(rows.reshape(slots, 2 * CAP, half))
    back = back.reshape(-1, half)
    gates = combine_gates(expert_ids, gate_fixed, slot_expert)
    base = own_sum(f_kept, own_came, shared_out)
    return mix(gates, back, base, (from_prev, from_next, from_far))


def solution(mesh):
    in_specs = (
        P(("dp", "expert"), "tensor"),
        P(("dp", "expert"), None),
        P(("dp", "expert"), None),
        P(),
        P(("dp", "expert"), "tensor", None, None),
        P(("dp", "expert"), None, "tensor"),
        P("tensor", None, "dp"),
        P("dp", "tensor"),
    )
    out_specs = P(("dp", "expert"), "tensor")
    return jax.shard_map(shards, mesh=mesh, in_specs=in_specs, out_specs=out_specs, check_vma=False)
```

```python
import functools

import jax
import jax.numpy as jnp
from jax import lax
from jax.experimental import pallas as pl
from jax.experimental.pallas import tpu as pltpu
from jax.sharding import PartitionSpec as P


CAP = 4
BF = jnp.bfloat16
F32 = jnp.float32


def params(mib=20):
    return pltpu.CompilerParams(vmem_limit_bytes=mib * 2**20)


def far(array):
    return pltpu.with_memory_space_constraint(array, pltpu.HBM)


def dot(a, b):
    return jnp.dot(a, b, preferred_element_type=F32)


def iota(shape, dim):
    return lax.broadcasted_iota(jnp.int32, shape, dim)


def silu_mul(gate, up):
    return (jax.nn.silu(gate) * up).astype(BF)


def served_lanes(ids, held_row):
    slots = held_row.shape[1]
    lanes = slots * 2 * CAP
    tokens = ids.shape[1]
    col, slot = iota((lanes, slots), 1), iota((lanes, slots), 0) >> 3
    held_all = jnp.broadcast_to(held_row[...], (lanes, slots))
    held = jnp.max(jnp.where(col == slot, held_all, -1), axis=1, keepdims=True)
    twin = (held_all == held) & (col < slot)
    spare = jnp.max(jnp.where(twin, CAP, 0), axis=1, keepdims=True)
    named = jnp.zeros((lanes, tokens), F32)
    for k in range(ids.shape[0]):
        named = jnp.where(ids[k : k + 1, :] == held, 1.0, named)
    earlier = iota((tokens, tokens), 0) < iota((tokens, tokens), 1)
    rank = dot(named.astype(BF), jnp.where(earlier, 1.0, 0.0).astype(BF))
    row = iota((lanes, 1), 0)
    place = (spare + (row & (CAP - 1))).astype(F32)
    served = (named > 0.5) & (rank == place)
    return served, held, (row & CAP) == 0


def route_kernel(ids, held_row, left, right, rows_out, pick):
    @pl.when(pl.program_id(0) == 0)
    def _():
        served, _, is_left = served_lanes(ids, held_row)
        one = jnp.where(served, 1.0, 0.0)
        pick[0] = jnp.where(is_left, one, 0.0).astype(BF)
        pick[1] = jnp.where(is_left, 0.0, one).astype(BF)

    rows_out[...] = (dot(pick[0], left[...]) + dot(pick[1], right[...])).astype(BF)


def whole_of(array):
    return pl.BlockSpec(array.shape, lambda *_: (0,) * array.ndim)


def route(ids, slot_expert, hidden, block=768):
    slots = slot_expert.shape[0]
    lanes = slots * 2 * CAP
    tokens, width = hidden.shape
    half = width // 2
    blocks = half // block
    ids, held = ids.T, slot_expert[None]
    return pl.pallas_call(
        route_kernel,
        grid=(blocks,),
        in_specs=[
            whole_of(ids),
            whole_of(held),
            pl.BlockSpec((tokens, block), lambda j: (0, j)),
            pl.BlockSpec((tokens, block), lambda j: (0, blocks + j)),
        ],
        out_specs=pl.BlockSpec((lanes, block), lambda j: (0, j)),
        out_shape=pltpu.HBM((lanes, half), BF),
        scratch_shapes=[pltpu.VMEM((2, lanes, tokens), BF)],
        compiler_params=params(16),
        name="route",
    )(*(far(x) for x in (ids, held, hidden, hidden)))


def gates_kernel(ids, gates, held_row, out):
    served, held, is_left = served_lanes(ids, held_row)
    tokens = ids.shape[1]
    gate = jnp.zeros(served.shape, jnp.int32)
    for k in range(ids.shape[0]):
        gate = gate + jnp.where(ids[k : k + 1, :] == held, gates[k : k + 1, :], 0)
    gate = jnp.where(served, gate, 0)
    high = (gate >> 8).astype(F32) * 2.0**-8
    low = (gate & 255).astype(F32) * 2.0**-16
    for i, part in enumerate((high, low)):
        rows = slice(i * tokens, (i + 1) * tokens)
        out[0, rows, :] = jnp.where(is_left, part, 0.0).T.astype(BF)
        out[1, rows, :] = jnp.where(is_left, 0.0, part).T.astype(BF)


def combine_gates(ids, gates, slot_expert):
    lanes = slot_expert.shape[0] * 2 * CAP
    operands = ids.T, gates.T, slot_expert[None]
    shape = (2, 2 * ids.shape[0], lanes)
    return pl.pallas_call(
        gates_kernel,
        grid=(1,),
        in_specs=[whole_of(x) for x in operands],
        out_specs=pl.BlockSpec(shape, lambda j: (0, 0, 0)),
        out_shape=pltpu.HBM(shape, BF),
        compiler_params=params(16),
        name="combine_gates",
    )(*(far(x) for x in operands))


def split_kernel(w, w_shared, out, out_shared, *, sub):
    row, col = iota((2 * sub, 2 * sub), 0), iota((2 * sub, 2 * sub), 1)
    source = jnp.where(row < sub, 2 * row, 2 * (row - sub) + 1)
    order = jnp.where(col == source, 1.0, 0.0).astype(BF)
    block, part = out.shape[2], out_shared.shape[2] // 2
    for start in range(0, w.shape[0], sub):
        here = slice(start, start + sub)
        moved = dot(order, w[here].reshape(2 * sub, w.shape[2])).astype(BF)
        for j in range(2):
            cols = slice(j * block, (j + 1) * block)
            out[j, here, :] = moved[:sub, cols]
            out[2 + j, here, :] = moved[sub:, cols]
        moved = dot(order, w_shared[here].reshape(2 * sub, w_shared.shape[2])).astype(BF)
        for j in range(2):
            cols = slice(j * part, (j + 1) * part)
            out_shared[j, here, :part] = moved[:sub, cols]
            out_shared[j, here, part:] = moved[sub:, cols]


def split_gate_up(w, w_shared, depth=768, sub=128):
    width, _, units = w.shape
    shared_units = w_shared.shape[2]

    def taken(columns):
        return pl.BlockSpec((depth, 2, columns), lambda i: (i, 0, 0))

    def given(blocks, block):
        return pl.BlockSpec((blocks, depth, block), lambda i: (0, i, 0))

    return pl.pallas_call(
        functools.partial(split_kernel, sub=sub),
        grid=(width // depth,),
        in_specs=[taken(units), taken(shared_units)],
        out_specs=(given(4, units // 2), given(2, shared_units)),
        out_shape=(
            pltpu.HBM((4, width, units // 2), BF),
            pltpu.HBM((2, width, shared_units), BF),
        ),
        compiler_params=params(24),
        name="split",
    )(far(w), far(w_shared))


def fetch(w, held, sems, side):
    copies = []
    cut = w.shape[1] // 2
    for j in range(2):
        for k in range(2):
            rows = slice(k * cut, (k + 1) * cut)
            copies.append(
                pltpu.make_async_copy(
                    w.at[2 * j + side, rows], held.at[j, rows], sems.at[2 * j + k]
                )
            )
            copies[-1].start()
    return copies


def multiply(x, held, copies, out):
    cut, block = held.shape[1] // 2, held.shape[2]
    for j in range(2):
        total = None
        for k in range(2):
            copies[2 * j + k].wait()
            rows = slice(k * cut, (k + 1) * cut)
            part = dot(x[:, rows], held[j, rows])
            total = part if total is None else total + part
        out[:, j * block : (j + 1) * block] = total.astype(out.dtype)


def swap_halves(first, second):
    top = iota(first.shape, 1) < CAP
    lower = jnp.where(top, first, pltpu.roll(second, CAP, 1))
    upper = jnp.where(top, pltpu.roll(first, CAP, 1), second)
    return lower, upper


def send_kernel(me, arrived, w, x_out, out, held, sems, *, block=512):
    copies = fetch(w, held, sems, 1 - me[0])
    lanes, half = arrived.shape
    for start in range(0, half, block):
        tiles = arrived[:, start : start + block].astype(F32)
        tiles = tiles.reshape(lanes // 16, 2, 8, block)
        for h, part in enumerate(swap_halves(tiles[:, 0], tiles[:, 1])):
            cols = slice(h * half + start, h * half + start + block)
            x_out[:, cols] = part.reshape(lanes // 2, block).astype(BF)
    multiply(x_out, held, copies, out)


def weight_scratch(w):
    return [pltpu.VMEM((2, *w.shape[1:]), BF), pltpu.SemaphoreType.DMA((4,))]


def send_half(arrived, w, me):
    lanes, half = arrived.shape
    rows, units = lanes // 2, 2 * w.shape[2]
    near = pl.BlockSpec(memory_space=pltpu.VMEM)
    return pl.pallas_call(
        send_kernel,
        in_specs=[pl.BlockSpec(memory_space=pltpu.SMEM), near, pl.BlockSpec(memory_space=pl.ANY)],
        out_shape=(
            jax.ShapeDtypeStruct((rows, 2 * half), BF),
            jax.ShapeDtypeStruct((rows, units), BF),
        ),
        scratch_shapes=weight_scratch(w),
        compiler_params=params(),
        name="send_half",
    )(me, arrived, far(w))


def keep_kernel(me, x, w, out, held, sems):
    multiply(x, held, fetch(w, held, sems, me[0]), out)


def keep_half(x, w, me):
    near = pl.BlockSpec(memory_space=pltpu.VMEM)
    return pl.pallas_call(
        keep_kernel,
        in_specs=[pl.BlockSpec(memory_space=pltpu.SMEM), near, pl.BlockSpec(memory_space=pl.ANY)],
        out_shape=jax.ShapeDtypeStruct((x.shape[0], 2 * w.shape[2]), F32),
        scratch_shapes=weight_scratch(w),
        compiler_params=params(),
        name="keep_half",
    )(me, x, far(w))


def act_kernel(kept, came, out):
    units = out.shape[1]
    pre = kept[...] + came[...].astype(F32)
    out[...] = silu_mul(pre[:, :units], pre[:, units:])


def activate(kept, came):
    rows, units = kept.shape
    return pl.pallas_call(
        act_kernel,
        out_shape=jax.ShapeDtypeStruct((rows, units // 2), BF),
        compiler_params=params(),
        name="activate",
    )(kept, came)


def answer_kernel(me, mine, other, w, out, *, block):
    rows, units = mine.shape
    half = out.shape[1]
    at_mine = pl.ds(pl.multiple_of(me[0] * units, units), units)
    at_other = pl.ds(pl.multiple_of((1 - me[0]) * units, units), units)

    def answer(start):
        cols = slice(start, start + block)
        total = dot(mine[...], w[at_mine, cols]) + dot(other[...], w[at_other, cols])
        return total.reshape(rows // 8, 8, block)

    for start in range(0, half, block):
        parts = swap_halves(answer(start), answer(half + start))
        both = jnp.stack(parts, axis=1).reshape(2 * rows, block)
        out[:, start : start + block] = both.astype(BF)


def answers(mine, other, w, me, block=768):
    rows, _ = mine.shape
    near = pl.BlockSpec(memory_space=pltpu.VMEM)
    return pl.pallas_call(
        functools.partial(answer_kernel, block=block),
        in_specs=[pl.BlockSpec(memory_space=pltpu.SMEM)] + [near] * 3,
        out_shape=jax.ShapeDtypeStruct((2 * rows, w.shape[1] // 2), BF),
        compiler_params=params(),
        name="answers",
    )(me, mine, other, w)


def shared_kernel(*refs, count, cuts, ahead):
    pieces, w = refs[:count], refs[count]
    kept, *sent = refs[count + 1 : count + 2 + len(cuts)]
    pre = dot(jnp.concatenate([piece[...] for piece in pieces], axis=0), w[0])
    kept[...] = pre
    start = 0
    for rows, out in zip(cuts, sent):
        out[...] = pre[start : start + rows].astype(BF)
        start += rows
    if ahead:

        @pl.when(pl.program_id(0) == 0)
        def _():
            up, down = refs[-2:]
            rows = up.shape[0]
            up[...] = pieces[0][:rows, :]
            down[...] = pieces[1][rows:, :]


def shared_in_part(pieces, w, cuts, ahead=0):
    rows = sum(piece.shape[0] for piece in pieces)
    blocks, width, block = w.shape

    def part(rows):
        return pl.BlockSpec((rows, block), lambda j: (0, j))

    out_specs = [part(rows)] + [part(cut) for cut in cuts]
    out_shape = [pltpu.HBM((rows, blocks * block), F32)]
    out_shape += [jax.ShapeDtypeStruct((cut, blocks * block), BF) for cut in cuts]
    if ahead:
        out_specs += [pl.BlockSpec((ahead, width), lambda j: (0, 0))] * 2
        out_shape += [jax.ShapeDtypeStruct((ahead, width), BF)] * 2
    return pl.pallas_call(
        functools.partial(shared_kernel, count=len(pieces), cuts=cuts, ahead=ahead),
        grid=(blocks,),
        in_specs=[pl.BlockSpec(memory_space=pltpu.VMEM)] * len(pieces)
        + [pl.BlockSpec((1, width, block), lambda j: (j, 0, 0))],
        out_specs=tuple(out_specs),
        out_shape=tuple(out_shape),
        compiler_params=params(),
        name="shared_in",
    )(*pieces, far(w))


def paired_act(kept, came, block=256):
    pre = kept + came.astype(F32)
    half = block // 2
    return jnp.concatenate(
        [
            silu_mul(pre[:, j : j + half], pre[:, j + half : j + block])
            for j in range(0, pre.shape[1], block)
        ],
        axis=1,
    )


def out_kernel(kept, came, w, *outs):
    rows = outs[0].shape[0]
    total = dot(paired_act(kept[: came.shape[0], :], came[...]), w[...])
    for i, out in enumerate(outs):
        out[...] = total[i * rows : (i + 1) * rows].astype(BF)


def shared_out_part(kept, came, w, count):
    rows, width = came.shape[0] // count, w.shape[1]
    return pl.pallas_call(
        out_kernel,
        in_specs=[pl.BlockSpec(memory_space=pltpu.VMEM)] * 3,
        out_shape=(jax.ShapeDtypeStruct((rows, width), BF),) * count,
        compiler_params=params(),
        name="shared_out",
    )(kept, came, w)


def base_kernel(kept, came, w, out):
    out[...] = dot(paired_act(kept[...], came[...]), w[...])


def own_sum(kept, came, w, block=1536):
    units, width = w.shape
    tokens = came.shape[0]
    return pl.pallas_call(
        base_kernel,
        grid=(width // block,),
        in_specs=[
            pl.BlockSpec((tokens, kept.shape[1]), lambda j: (1, 0)),
            pl.BlockSpec(came.shape, lambda j: (0, 0)),
            pl.BlockSpec((units, block), lambda j: (0, j)),
        ],
        out_specs=pl.BlockSpec((tokens, block), lambda j: (0, j)),
        out_shape=pltpu.HBM((tokens, width), F32),
        compiler_params=params(),
        name="own_sum",
    )(far(kept), far(came), far(w))


def mix_kernel(gates, back, base, a, b, c, out):
    tokens = out.shape[0]
    total = base[...] + a[...].astype(F32) + b[...].astype(F32) + c[...].astype(F32)
    both = dot(gates[0], back[...])
    out[...] = (total + both[:tokens] + both[tokens:]).astype(BF)


def mix(gates, back, base, came, block=1536):
    _, both, lanes = gates.shape
    tokens, width = base.shape
    blocks = width // 2 // block
    part = pl.BlockSpec((tokens, block), lambda j: (0, j))
    return pl.pallas_call(
        mix_kernel,
        grid=(2 * blocks,),
        in_specs=[
            pl.BlockSpec((1, both, lanes), lambda j: (j // blocks, 0, 0)),
            pl.BlockSpec((lanes, block), lambda j: (0, j % blocks)),
        ]
        + [part] * 4,
        out_specs=part,
        out_shape=jax.ShapeDtypeStruct((tokens, width), BF),
        compiler_params=params(),
        name="mix",
    )(far(gates), back, far(base), *(far(x) for x in came))


def shift(array, axis, by):
    size = lax.axis_size(axis)
    return lax.ppermute(array, axis, [(i, (i + by) % size) for i in range(size)])


def exchange(rows):
    return lax.all_to_all(rows, ("dp", "expert"), split_axis=0, concat_axis=0, tiled=True)


def shards(
    hidden, expert_ids, gate_fixed, slot_expert, expert_in, expert_out, shared_in, shared_out
):
    tokens, width = hidden.shape
    slots = slot_expert.shape[0]
    half = width // 2
    me = lax.axis_index("tensor").astype(jnp.int32)[None]

    prev = shift(hidden, "dp", 1)
    nxt = shift(hidden, "dp", -1)
    send_rows = route(expert_ids, slot_expert, hidden)
    arrived = exchange(send_rows.reshape(slots, 2 * CAP, half))
    arrived = arrived.reshape(-1, half)
    w_in, w_shared = split_gate_up(expert_in[0], shared_in)
    n_kept, n_sent, ahead, behind = shared_in_part(
        (prev, nxt), w_shared, (2 * tokens,), tokens // 2
    )
    n_came = shift(n_sent, "tensor", 1)
    far_a = shift(ahead, "dp", 1)
    far_b = shift(behind, "dp", -1)

    x, sent = send_half(arrived, w_in, me)
    came = shift(sent, "tensor", 1)
    kept = keep_half(x, w_in, me)
    down, up = shared_out_part(n_kept, n_came, shared_out, 2)
    from_prev = shift(up, "dp", 1)
    from_next = shift(down, "dp", -1)
    f_kept, f_sent, own_sent = shared_in_part(
        (far_a, far_b, hidden), w_shared, (tokens, tokens)
    )
    f_came = shift(f_sent, "tensor", 1)
    own_came = shift(own_sent, "tensor", 1)

    act = activate(kept, came)
    act_other = shift(act, "tensor", 1)
    (far_part,) = shared_out_part(f_kept, f_came, shared_out, 1)
    from_far = shift(far_part, "dp", 2)

    rows = answers(act, act_other, expert_out[0], me)
    back = exchange(rows.reshape(slots, 2 * CAP, half))
    back = back.reshape(-1, half)
    gates = combine_gates(expert_ids, gate_fixed, slot_expert)
    base = own_sum(f_kept, own_came, shared_out)
    return mix(gates, back, base, (from_prev, from_next, from_far))


def solution(mesh):
    in_specs = (
        P(("dp", "expert"), "tensor"),
        P(("dp", "expert"), None),
        P(("dp", "expert"), None),
        P(),
        P(("dp", "expert"), "tensor", None, None),
        P(("dp", "expert"), None, "tensor"),
        P("tensor", None, "dp"),
        P("dp", "tensor"),
    )
    out_specs = P(("dp", "expert"), "tensor")
    return jax.shard_map(shards, mesh=mesh, in_specs=in_specs, out_specs=out_specs, check_vma=False)
```
